32 devices in a mesh: dp: 2 (over x), fsdp: 16 (over z, y, core).
Axes of the slice: x: 2, y: 2, z: 4, core: 2. Of those that a mesh axis runs over, the one named last changes fastest.
Arguments:
- tokens: bfloat16 [32, 256, 3584], P(('dp', 'fsdp')), may hold values from -11 to 11
- queries: bfloat16 [32, 256, 1792], P(('dp', 'fsdp')), may hold values from -48 to 48
- key_weight: bfloat16 [3584, 256], P('fsdp'), may hold values from -0.09375 to 0.09375
- value_weight: bfloat16 [3584, 256], P('fsdp'), may hold values from -0.09375 to 0.09375
- key_variance: float32 [3584, 256], P('fsdp'), may hold values from 0.00069754466 to 0.013950893
- sign_bits: int32 [3584, 35], P('fsdp'), may hold values from 0 to 1073741823
Outputs:
- attended: bfloat16 [32, 256, 1792], P(('dp', 'fsdp'))
- spread: bfloat16 [32, 256, 1792], P(('dp', 'fsdp'))
- head_mean: float32 [14], replicated
The draws below stay inside these ranges and needn't reach their ends.
All inputs are finite; a program needn't handle non-finite values.
Results may differ from the reference program's by a relative error of at most 0.014.
The reference program's roundings to bfloat16 on the way (of `tangent`) count: a program that leaves them out, or rounds other values in their place, can miss the bound.
Values may be sent and summed in bfloat16 or wider, within the bound.
No kernel may reach another device: no remote copies, remote signals or barrier semaphores. Data moves between devices by JAX's collectives and lax.ppermute only.
A program may use at most 128 MiB of HBM per device.

```python
import math
import jax
import jax.numpy as jnp
import numpy as np
from jax import lax

D = 3584
HD = 128
KVH = 2
QPK = 7
TANG = 4
LEN = 256
HEADS = 14
KVW = 256
WORDS = 35
SEQS = 32


def draw_tokens(key, part):
    base = jnp.clip(jax.random.normal(key, (SEQS, LEN, D), jnp.float32), -6.0, 6.0)
    order = jnp.arange(SEQS, dtype=jnp.float32) / max(SEQS - 1, 1)
    growth = 3.0 ** (0.25 * order)
    return (base * growth[:, None, None]).astype(jnp.bfloat16)


def draw_queries(key, part):
    base = jnp.clip(jax.random.normal(key, (SEQS, LEN, HEADS, HD), jnp.float32), -6.0, 6.0)
    return base.reshape(SEQS, LEN, HEADS * HD).astype(jnp.bfloat16)


def touch_ends(entries, own_key, low, largest):
    longest = entries.shape.index(max(entries.shape))
    spots = []
    for shift in (0, 1):
        where = [jax.random.randint(jax.random.fold_in(own_key, axis), (), 0, length) for axis, length in enumerate(entries.shape)]
        where[longest] = (where[longest] + shift) % entries.shape[longest]
        spots.append(tuple(where))
    return entries.at[spots[0]].set(low).at[spots[1]].set(largest)


def block_levels(stream_key, extent, split, least, largest):
    loudness = 1.0
    for dim, blocks in split:
        heights = jax.random.uniform(jax.random.fold_in(jax.random.fold_in(stream_key, 6), dim), (blocks,), jnp.float32, least / len(split), largest / len(split))
        loudness = loudness * jnp.repeat(jnp.exp(heights), extent[dim] // blocks).reshape((-1,) + (1,) * (len(extent) - 1 - dim))
    return loudness


def scatter_about(stream_key, shape, scale, reach, split=(), held_as=jnp.bfloat16):
    array = scale * jax.random.normal(stream_key, shape, jnp.float32)
    if split:
        array = array * block_levels(stream_key, shape, split, -0.22, 0.18)
    return jnp.clip(array, -reach, reach).astype(held_as)


def setup_inputs(seed: int = 0) -> dict:
    key_of = jax.random.split(jax.random.key(seed), 7)
    return {
        "tokens": draw_tokens(jax.random.fold_in(key_of[6], 71), 0),
        "queries": draw_queries(jax.random.fold_in(key_of[6], 71), 0),
        "key_weight": scatter_about(key_of[2], (D, KVW), D ** -0.5, 0.09375, ((0, 16),)),
        "value_weight": scatter_about(key_of[3], (D, KVW), D ** -0.5, 0.09375, ((0, 16),)),
        "key_variance": jnp.clip(jnp.exp(math.log(0.013950893) - 2.9957322 * jax.random.uniform(key_of[4], (D, KVW), jnp.float32) ** block_levels(key_of[4], (D, KVW), ((0, 16),), -0.2, 0.2)), 0.00069754466, 0.013950893),
        "sign_bits": touch_ends(jax.random.randint(key_of[5], (D, WORDS), 0, 1073741824), jax.random.fold_in(key_of[5], 1), 0, 1073741823).astype(jnp.int32),
    }


word_bits = 30

def sign_table(packed, columns):
    position = np.arange(columns)
    chosen = jnp.take(packed, jnp.asarray(position // word_bits, jnp.int32), axis=1)
    shifted = jnp.right_shift(chosen, jnp.asarray(position % word_bits, jnp.int32))
    return (2 * jnp.bitwise_and(shifted, 1) - 1).astype(jnp.float32)

def make_tangent(key_variance, sign_bits):
    root = jnp.sqrt(key_variance).astype(jnp.bfloat16)
    tiled = jnp.tile(root, (1, TANG)).astype(jnp.float32)
    return (tiled * sign_table(sign_bits, TANG * KVH * HD)).astype(jnp.bfloat16)

def attend(query_rows, key_rows, value_rows, tangent_keys):
    length = query_rows.shape[0]
    factor = HD ** (-0.5)
    causal = jnp.arange(length)[:, None] >= jnp.arange(length)[None, :]
    outputs = []
    spreads = []
    tangent_split = tangent_keys.reshape(length, TANG, KVH, HD)
    for group in range(KVH):
        query_group = query_rows[:, group * QPK * HD:(group + 1) * QPK * HD].reshape(length, QPK, HD).astype(jnp.float32)
        key_group = key_rows[:, group * HD:(group + 1) * HD].astype(jnp.float32)
        value_group = value_rows[:, group * HD:(group + 1) * HD].astype(jnp.float32)
        tangent_group = tangent_split[:, :, group, :].astype(jnp.float32)
        scores = jnp.einsum('qhd,kd->hqk', query_group, key_group) * factor
        scores = jnp.where(causal, scores, -jnp.inf)
        raised = jnp.exp(scores - lax.optimization_barrier(jnp.max(scores, axis=-1, keepdims=True)))
        weights = raised / lax.optimization_barrier(jnp.sum(raised, axis=-1, keepdims=True))
        rounded = weights.astype(jnp.bfloat16).astype(jnp.float32)
        outputs.append(jnp.einsum('hqk,kd->qhd', rounded, value_group).reshape(length, QPK * HD))
        moved = jnp.einsum('qhd,ktd->thqk', query_group, tangent_group) * factor
        centred = weights * (moved - lax.optimization_barrier(jnp.sum(weights * moved, axis=-1, keepdims=True)))
        centred_rounded = centred.astype(jnp.bfloat16).astype(jnp.float32)
        response = jnp.einsum('thqk,kd->tqhd', centred_rounded, value_group)
        spreads.append((lax.optimization_barrier(jnp.sum(response * response, axis=0)) / TANG).reshape(length, QPK * HD))
    return (jnp.concatenate(outputs, axis=1), jnp.concatenate(spreads, axis=1))

def reference(tokens, queries, key_weight, value_weight, key_variance, sign_bits):
    tangent = make_tangent(key_variance, sign_bits)

    def one_sequence(pair):
        token_rows, query_rows = pair
        key_rows = jnp.dot(token_rows, key_weight, preferred_element_type=jnp.float32).astype(jnp.bfloat16)
        value_rows = jnp.dot(token_rows, value_weight, preferred_element_type=jnp.float32).astype(jnp.bfloat16)
        tangent_keys = jnp.dot(token_rows, tangent, preferred_element_type=jnp.float32).astype(jnp.bfloat16)
        attended, variance = attend(query_rows, key_rows, value_rows, tangent_keys)
        head_sums = lax.optimization_barrier(jnp.sum(variance.reshape(-1, HEADS, HD), axis=(0, 2)))
        return (attended.astype(jnp.bfloat16), variance.astype(jnp.bfloat16), head_sums)
    attended, spread, head_sums = lax.map(one_sequence, (tokens, queries))
    head_mean = lax.optimization_barrier(jnp.sum(head_sums, axis=0)) / (SEQS * LEN * HD)
    return (attended, spread, head_mean)
```

```python
import functools

import jax
import jax.numpy as jnp
import numpy as np
from jax import lax
from jax.experimental import pallas as pl
from jax.experimental.pallas import tpu as pltpu
from jax.sharding import PartitionSpec as P

HD = 128
KVH = 2
QPK = 7
TANG = 4
AXES = ("dp", "fsdp")
word_bits = 30


class Grid:
    def __init__(self, mesh):
        self.dp = mesh.shape["dp"]
        fsdp = mesh.shape["fsdp"]
        self.cores = 2 if fsdp % 2 == 0 else 1
        rest = fsdp // self.cores
        self.z = 4 if rest % 4 == 0 else 1
        self.y = rest // self.z
        self.count = self.dp * fsdp

    def index(self, d, z, y, c):
        return ((d * self.z + z) * self.y + y) * self.cores + c

    def move(self, value, to):
        pairs = []
        for d in range(self.dp):
            for z in range(self.z):
                for y in range(self.y):
                    for c in range(self.cores):
                        pairs.append((self.index(d, z, y, c), self.index(*to(d, z, y, c))))
        return lax.ppermute(value, AXES, pairs)

    def along_z(self, value, k):
        return self.move(value, lambda d, z, y, c: (d, z ^ k, y, c))

    def along_y(self, value, k):
        return self.move(value, lambda d, z, y, c: (d, z, (y + k) % self.y, c))

    def along_x(self, value):
        return self.move(value, lambda d, z, y, c: (d ^ 1, z, y, c))

    def across(self, value):
        return self.move(value, lambda d, z, y, c: (d, z, y, 1 - c))


def sign_codes(packed):
    position = np.arange(TANG * KVH * HD)
    chosen = jnp.take(packed, jnp.asarray(position // word_bits, jnp.int32), axis=1)
    bits = jnp.bitwise_and(
        jnp.right_shift(chosen, jnp.asarray(position % word_bits, jnp.int32)), 1
    )
    scale = jnp.asarray(1 << (position // HD), jnp.int32)
    return jnp.sum((bits * scale).reshape(packed.shape[0], TANG * KVH, HD), axis=1)


def gather(grid, first, second, halve):
    half = first.shape[0] // 2
    if halve:
        sent = lax.dynamic_slice_in_dim(first, (lax.axis_index("dp") % 2) * half, half, 0)
    else:
        sent = first
    slots_a = {(k, 0): sent for k in range(1)}
    slots_b = {(0, 0): second}
    for k in range(1, grid.z):
        slots_a[(k, 0)] = grid.along_z(sent, k)
    for k in range(1, grid.z):
        slots_b[(k, 0)] = grid.along_z(second, k)
    for e in range(1, grid.y):
        for k in range(grid.z):
            slots_a[(k, e)] = grid.along_y(slots_a[(k, 0)], e)
    whole = {(0, 0): (first,)}
    for key, value in slots_a.items():
        if key != (0, 0):
            whole[key] = (value, grid.along_x(value)) if halve else (value,)
    for e in range(1, grid.y):
        for k in range(grid.z):
            slots_b[(k, e)] = grid.along_y(slots_b[(k, 0)], e)
    out_a, out_b = [], []
    for key, parts in whole.items():
        out_a.append((parts, key + (0,)))
        if grid.cores == 2:
            out_a.append((tuple(grid.across(p) for p in parts), key + (1,)))
    for key, value in slots_b.items():
        out_b.append(((value,), key + (0,)))
        if grid.cores == 2:
            out_b.append(((grid.across(value),), key + (1,)))
    return out_a, out_b


def owner(grid, key):
    me = lax.axis_index("fsdp")
    c = me % grid.cores
    y = (me // grid.cores) % grid.y
    z = me // (grid.cores * grid.y)
    k, e, dc = key
    return (jnp.bitwise_xor(z, k) * grid.y + (y - e) % grid.y) * grid.cores + (
        jnp.bitwise_xor(c, dc)
    )


def kernel(shapes, table, tokens, queries, *rest):
    counts_a, counts_b, rows = shapes
    slots = len(counts_a)
    n_a, n_b = sum(counts_a), sum(counts_b)
    in_a, in_b = rest[:n_a], rest[n_a : n_a + n_b]
    (
        att_ref,
        spread_ref,
        sums_ref,
        first,
        second,
        tangent,
        totals,
        rounded,
        sem_a,
        sem_b,
    ) = rest[n_a + n_b :]
    length = tokens.shape[1]
    block = HD
    group = pl.program_id(0)
    kvw = KVH * HD

    @pl.when(group == 0)
    def _project():
        mine = table[2 * slots]
        half = rows // 2
        at = 0
        for i, count in enumerate(counts_a):
            if count == 1:
                pltpu.make_async_copy(in_a[at], first.at[i], sem_a.at[i]).start()
            else:
                for j, where in enumerate((mine * half, (1 - mine) * half)):
                    pltpu.make_async_copy(
                        in_a[at + j],
                        first.at[i, pl.ds(pl.multiple_of(where, half), half)],
                        sem_a.at[i],
                    ).start()
            at += count
        for i in range(slots):
            pltpu.make_async_copy(in_b[i], second.at[i], sem_b.at[i]).start()
        totals[...] = jnp.zeros_like(totals)

        def add(i, carry):
            pltpu.make_async_copy(first.at[i], first.at[i], sem_a.at[i]).wait()
            root = first[i, :, :kvw].astype(jnp.float32)
            codes = first[i, :, kvw : kvw + HD].astype(jnp.float32).astype(jnp.int32)
            for t in range(TANG):
                for g in range(KVH):
                    part = root[:, g * HD : (g + 1) * HD]
                    keep = jnp.bitwise_and(codes, 1 << (KVH * t + g)) != 0
                    lane = t * kvw + g * HD
                    tangent[:, lane : lane + HD] = jnp.where(keep, part, -part).astype(
                        jnp.bfloat16
                    )
            rows_a = tokens[table[i]]
            totals[:, :kvw] += jnp.dot(
                rows_a, first[i, :, kvw + HD :], preferred_element_type=jnp.float32
            )
            totals[:, 2 * kvw :] += jnp.dot(
                rows_a, tangent[...], preferred_element_type=jnp.float32
            )
            pltpu.make_async_copy(second.at[i], second.at[i], sem_b.at[i]).wait()
            rows_b = tokens[table[slots + i]]
            totals[:, kvw : 2 * kvw] += jnp.dot(
                rows_b, second[i], preferred_element_type=jnp.float32
            )
            return carry

        lax.fori_loop(0, slots, add, 0)
        total = totals[...].astype(jnp.bfloat16)
        for g in range(KVH):
            for n in range(2 + TANG):
                rounded[g, n] = total[:, n * kvw + g * HD : n * kvw + (g + 1) * HD]

    factor = HD ** (-0.5)
    contract = (((1,), (1,)), ((), ()))

    def head(m, carry):
        lanes = pl.ds(pl.multiple_of(m * HD, HD), HD)
        sums = jnp.zeros((1, HD), jnp.float32)
        for b in range(length // block):
            rows_q = pl.ds(b * block, block)
            keys = (b + 1) * block
            query = queries[rows_q, lanes]
            scores = (
                lax.dot_general(
                    query, rounded[group, 0, :keys], contract, preferred_element_type=jnp.float32
                )
                * factor
            )
            q_at = b * block + lax.broadcasted_iota(jnp.int32, (block, keys), 0)
            k_at = lax.broadcasted_iota(jnp.int32, (block, keys), 1)
            scores = jnp.where(k_at <= q_at, scores, -1e30)
            raised = jnp.exp(scores - jnp.max(scores, axis=-1, keepdims=True))
            weights = raised * (1.0 / jnp.sum(raised, axis=-1, keepdims=True))
            values = rounded[group, 1, :keys]
            att_ref[rows_q, lanes] = jnp.dot(
                weights.astype(jnp.bfloat16), values, preferred_element_type=jnp.float32
            ).astype(att_ref.dtype)
            scaled = weights * factor
            variance = jnp.zeros((block, HD), jnp.float32)
            for t in range(TANG):
                moved = scaled * lax.dot_general(
                    query,
                    rounded[group, 2 + t, :keys],
                    contract,
                    preferred_element_type=jnp.float32,
                )
                centred = moved - weights * jnp.sum(moved, axis=-1, keepdims=True)
                response = jnp.dot(
                    centred.astype(jnp.bfloat16), values, preferred_element_type=jnp.float32
                )
                variance += response * response
            variance = variance * (1.0 / TANG)
            spread_ref[rows_q, lanes] = variance.astype(spread_ref.dtype)
            sums += jnp.sum(variance, axis=0, keepdims=True)
        sums_ref[0, pl.ds(m, 1), :] = sums
        return carry

    lax.fori_loop(0, QPK, head, 0)


def attend(grid, tokens, queries, pieces_a, pieces_b, halve):
    length = queries.shape[0]
    n, _, rows = tokens.shape
    slots = len(pieces_a)
    counts_a = tuple(len(parts) for parts, _ in pieces_a)
    counts_b = tuple(len(parts) for parts, _ in pieces_b)
    flat_a = [p for parts, _ in pieces_a for p in parts]
    flat_b = [p for parts, _ in pieces_b for p in parts]
    table = jnp.stack(
        [owner(grid, key) for _, key in pieces_a]
        + [owner(grid, key) for _, key in pieces_b]
        + [lax.axis_index("dp") % 2]
    ).astype(jnp.int32)
    kvw = KVH * HD
    wide_a, wide_b = flat_a[0].shape[1], flat_b[0].shape[1]
    anywhere = pl.BlockSpec(memory_space=pl.ANY)
    columns = QPK * HD
    return pl.pallas_call(
        functools.partial(kernel, (counts_a, counts_b, rows)),
        grid=(KVH,),
        in_specs=[
            pl.BlockSpec(memory_space=pltpu.SMEM),
            pl.BlockSpec((n, length, rows), lambda g: (0, 0, 0)),
            pl.BlockSpec((length, columns), lambda g: (0, g)),
        ]
        + [anywhere] * (len(flat_a) + len(flat_b)),
        out_specs=[
            pl.BlockSpec((length, columns), lambda g: (0, g)),
            pl.BlockSpec((length, columns), lambda g: (0, g)),
            pl.BlockSpec((1, 8, HD), lambda g: (g, 0, 0)),
        ],
        out_shape=[
            jax.ShapeDtypeStruct((length, KVH * columns), jnp.bfloat16),
            jax.ShapeDtypeStruct((length, KVH * columns), jnp.bfloat16),
            jax.ShapeDtypeStruct((KVH, 8, HD), jnp.float32),
        ],
        scratch_shapes=[
            pltpu.VMEM((slots, rows, wide_a), jnp.bfloat16),
            pltpu.VMEM((slots, rows, wide_b), jnp.bfloat16),
            pltpu.VMEM((rows, TANG * kvw), jnp.bfloat16),
            pltpu.VMEM((length, (2 + TANG) * kvw), jnp.float32),
            pltpu.VMEM((KVH, 2 + TANG, length, HD), jnp.bfloat16),
            pltpu.SemaphoreType.DMA((slots,)),
            pltpu.SemaphoreType.DMA((slots,)),
        ],
        compiler_params=pltpu.CompilerParams(
            dimension_semantics=("arbitrary",), vmem_limit_bytes=48 * 1024 * 1024
        ),
        cost_estimate=pl.CostEstimate(
            flops=6_000_000_000, bytes_accessed=20_000_000, transcendentals=1_000_000
        ),
    )(table, tokens, queries, *flat_a, *flat_b)


def reduce_all(grid, value):
    if grid.count & (grid.count - 1):
        return lax.psum(value, AXES)
    step = 1
    while step < grid.count:
        pairs = [(i, i ^ step) for i in range(grid.count)]
        value = value + lax.ppermute(value, AXES, pairs)
        step *= 2
    return value


def body(grid, tokens, queries, key_weight, value_weight, key_variance, sign_bits):
    token_rows = tokens[0]
    length, wide = token_rows.shape
    rows = key_weight.shape[0]
    halve = grid.dp % 2 == 0 and rows % 32 == 0
    root = jnp.sqrt(key_variance).astype(jnp.bfloat16)
    codes = sign_codes(sign_bits).astype(jnp.bfloat16)
    first = jnp.concatenate([root, codes, key_weight], axis=1)
    pieces_a, pieces_b = gather(grid, first, value_weight, halve)
    blocks = jnp.transpose(token_rows.reshape(length, wide // rows, rows), (1, 0, 2))
    attended, spread, sums = attend(grid, blocks, queries[0], pieces_a, pieces_b, halve)
    totals = reduce_all(grid, sums)
    count = grid.count * length * HD
    head_mean = jnp.sum(totals[:, :QPK], axis=2).reshape(-1) / count
    return attended[None], spread[None], head_mean


def solution(mesh):
    placed = (
        P(AXES, None, None),
        P(AXES, None, None),
        P("fsdp", None),
        P("fsdp", None),
        P("fsdp", None),
        P("fsdp", None),
    )
    return jax.shard_map(
        functools.partial(body, Grid(mesh)),
        mesh=mesh,
        in_specs=placed,
        out_specs=(P(AXES, None, None), P(AXES, None, None), P()),
        check_vma=False,
    )
```
